128 devices in a mesh: south: 16 (over z, y), east: 4 (over x), down: 2 (over core).
Axes of the slice: x: 4, y: 4, z: 4, core: 2. Of those that a mesh axis runs over, the one named last changes fastest.
Arguments:
- initial_scalar_state: float32 [64, 128, 256, 128], P('south', 'east', 'down'), may hold values from 0.2 to 1.8
- scaled_wind_second: float32 [64, 128, 256, 128], P('south', 'east', 'down'), may hold values from -0.3 to 0.3
- scaled_wind_first: float32 [64, 128, 256, 128], P('south', 'east', 'down'), may hold values from -0.3 to 0.3
- scaled_wind_third: float32 [64, 128, 256, 128], P('south', 'east', 'down'), may hold values from -0.3 to 0.3
Outputs:
- temperature_end: float32 [64, 128, 256, 128], P('south', 'east', 'down')
The draws below stay inside these ranges and needn't reach their ends.
All inputs are finite; a program needn't handle non-finite values.
Results may differ from the reference program's by a relative error of at most 0.00002.
Values sent between devices are 32-bit elements; how exact they have to be, the bound alone decides.
A program may use at most 448 MiB of HBM per device.

```python
import jax
import jax.numpy as jnp
from jax import lax

SECOND_AXIS_SIZE = 64
FIRST_AXIS_SIZE = 128
THIRD_AXIS_SIZE = 256
HEIGHT_COUNT = 128
STEPS = 4


def steps_of(stream_key, extent, split, low, largest):
    gain, own = 1.0, jax.random.fold_in(stream_key, 6)
    for axis_at, shards_of in split:
        steps = jnp.exp(jax.random.uniform(jax.random.fold_in(own, axis_at), (shards_of,), jnp.float32, low / len(split), largest / len(split)))
        gain = gain * jnp.repeat(steps, extent[axis_at] // shards_of).reshape([-1 if axis == axis_at else 1 for axis in range(len(extent))])
    return gain


def setup_inputs(seed: int = 0) -> dict:
    arg_keys = jax.random.split(jax.random.key(seed), 5)
    initial_scalar_state = jnp.clip(0.2 + 1.5999999 * jax.random.uniform(arg_keys[0], (SECOND_AXIS_SIZE, FIRST_AXIS_SIZE, THIRD_AXIS_SIZE, HEIGHT_COUNT), jnp.float32) ** steps_of(arg_keys[0], (SECOND_AXIS_SIZE, FIRST_AXIS_SIZE, THIRD_AXIS_SIZE, HEIGHT_COUNT), ((0, 16), (1, 4), (2, 2)), -0.2, 0.2), 0.2, 1.8)
    scaled_wind_second = jnp.clip(jax.random.uniform(arg_keys[1], (SECOND_AXIS_SIZE, FIRST_AXIS_SIZE, THIRD_AXIS_SIZE, HEIGHT_COUNT), jnp.float32, -0.3, 0.3) * steps_of(arg_keys[1], (SECOND_AXIS_SIZE, FIRST_AXIS_SIZE, THIRD_AXIS_SIZE, HEIGHT_COUNT), ((0, 16), (1, 4), (2, 2)), -0.4, 0.0), -0.3, 0.3)
    scaled_wind_first = jnp.clip(jax.random.uniform(arg_keys[2], (SECOND_AXIS_SIZE, FIRST_AXIS_SIZE, THIRD_AXIS_SIZE, HEIGHT_COUNT), jnp.float32, -0.3, 0.3) * steps_of(arg_keys[2], (SECOND_AXIS_SIZE, FIRST_AXIS_SIZE, THIRD_AXIS_SIZE, HEIGHT_COUNT), ((0, 16), (1, 4), (2, 2)), -0.4, 0.0), -0.3, 0.3)
    scaled_wind_third = jnp.clip(jax.random.uniform(arg_keys[3], (SECOND_AXIS_SIZE, FIRST_AXIS_SIZE, THIRD_AXIS_SIZE, HEIGHT_COUNT), jnp.float32, -0.3, 0.3) * steps_of(arg_keys[3], (SECOND_AXIS_SIZE, FIRST_AXIS_SIZE, THIRD_AXIS_SIZE, HEIGHT_COUNT), ((0, 16), (1, 4), (2, 2)), -0.4, 0.0), -0.3, 0.3)
    return {"initial_scalar_state": initial_scalar_state, "scaled_wind_second": scaled_wind_second, "scaled_wind_first": scaled_wind_first, "scaled_wind_third": scaled_wind_third}


def strip_edges(values, dims):
    for dim in dims:
        values = lax.slice_in_dim(values, 1, values.shape[dim] - 1, axis=dim)
    return values


def neighbour(values, dim, start, dims):
    others = [other for other in dims if other != dim]
    values = strip_edges(values, others)
    return lax.slice_in_dim(values, start, start + values.shape[dim] - 2, axis=dim)


def update_lone_timestep(padded_with_margin, scaled_wind_second, scaled_wind_first, scaled_wind_third):
    middle = strip_edges(padded_with_margin, (0, 1, 2))
    lower = [neighbour(padded_with_margin, dim, 0, (0, 1, 2)) for dim in (0, 1, 2)]
    upper = [neighbour(padded_with_margin, dim, 2, (0, 1, 2)) for dim in (0, 1, 2)]
    slopes = [above - below for above, below in zip(upper, lower)]
    smooth_rate = 0.05
    spread = lower[0] + upper[0] + lower[1] + upper[1] + lower[2] + upper[2] - 6.0 * middle
    return middle - scaled_wind_second * slopes[0] - scaled_wind_first * slopes[1] - scaled_wind_third * slopes[2] + smooth_rate * spread


def reference(initial_scalar_state, scaled_wind_second, scaled_wind_first, scaled_wind_third):
    for step in range(STEPS):
        initial_scalar_state = update_lone_timestep(jnp.pad(initial_scalar_state, ((1, 1), (1, 1), (1, 1), (0, 0)), mode="wrap"), scaled_wind_second, scaled_wind_first, scaled_wind_third)
    return initial_scalar_state
```

```python
import functools

import jax
import jax.numpy as jnp
from jax import lax
from jax.experimental import pallas as pl
from jax.experimental.pallas import tpu as pltpu
from jax.sharding import PartitionSpec as P

STEPS = 4
CHUNKS = 8
PAD = 8
MESH = pl.DeviceIdType.MESH
SMOOTH = 0.05


def kernel(
    sizes,
    x_hbm,
    wind_south_hbm,
    wind_east_hbm,
    wind_down_hbm,
    out_hbm,
    state,
    winds,
    load_sem,
    south_send,
    south_recv,
    east_send,
    east_recv,
    down_send,
    down_recv,
    out_sem,
):
    n_south, n_east, n_down = sizes
    planes, rows, depth, _ = x_hbm.shape
    per = rows // CHUNKS
    middle = pl.ds(PAD, depth)
    own_planes = pl.ds(1, planes)

    me_south, me_east, me_down = (lax.axis_index(a) for a in ("south", "east", "down"))
    above = {"south": lax.rem(me_south + 1, n_south)}
    below = {"south": lax.rem(me_south + n_south - 1, n_south)}
    right = {"east": lax.rem(me_east + 1, n_east)}
    left = {"east": lax.rem(me_east + n_east - 1, n_east)}
    partner = {"down": lax.rem(me_down + 1, n_down)}

    loads = []
    for a, ref in enumerate((x_hbm, wind_south_hbm, wind_east_hbm, wind_down_hbm)):
        for p in range(planes):
            target = state.at[0, 1 + p, pl.ds(1, rows), middle] if a == 0 else winds.at[a - 1, p]
            loads.append(pltpu.make_async_copy(ref.at[p], target, load_sem.at[a, p]))
    for load in loads:
        load.start()

    barrier = pltpu.get_barrier_semaphore()
    for neighbour in (above, below, right, left, partner):
        pl.semaphore_signal(barrier, inc=1, device_id=neighbour, device_id_type=MESH)
    pl.semaphore_wait(barrier, 5)

    def remote(src, dst, send, recv, device):
        return pltpu.make_async_remote_copy(
            src_ref=src, dst_ref=dst, send_sem=send, recv_sem=recv, device_id=device, device_id_type=MESH
        )

    def south_copies(n, c):
        slot = n % 2
        here = pl.ds(1 + c * per, per)
        result = []
        for way, (p, halo, device) in enumerate(((planes, 0, above), (1, planes + 1, below))):
            if n == 0:
                src = x_hbm.at[p - 1, pl.ds(c * per, per)]
            else:
                src = state.at[slot, p, here, middle]
            result.append(
                remote(
                    src,
                    state.at[slot, halo, here, middle],
                    south_send.at[way, n, c],
                    south_recv.at[way, n, c],
                    device,
                )
            )
        return result

    def east_copy(n, way):
        slot = n % 2
        r, halo, device = ((rows, 0, right), (1, rows + 1, left))[way]
        src = x_hbm.at[:, r - 1] if n == 0 else state.at[slot, own_planes, r, middle]
        return remote(
            src, state.at[slot, own_planes, halo, middle], east_send.at[way, n], east_recv.at[way, n], device
        )

    def down_copies(n, c):
        slot = n % 2
        here = pl.ds(1 + c * per, per)
        result = []
        for way, (k, halo) in enumerate(((depth - PAD, 0), (0, depth + PAD))):
            if n == 0:
                src = x_hbm.at[:, pl.ds(c * per, per), pl.ds(k, PAD)]
            else:
                src = state.at[slot, own_planes, here, pl.ds(PAD + k, PAD)]
            result.append(
                remote(
                    src,
                    state.at[slot, own_planes, here, pl.ds(halo, PAD)],
                    down_send.at[way, n, c],
                    down_recv.at[way, n, c],
                    partner,
                )
            )
        return result

    def out_copy(c):
        return pltpu.make_async_copy(
            state.at[STEPS % 2, own_planes, pl.ds(1 + c * per, per), middle],
            out_hbm.at[:, pl.ds(c * per, per)],
            out_sem.at[c],
        )

    def compute(n, c, which):
        now, later = n % 2, (n + 1) % 2

        def row(i, carry):
            r = c * per + i
            q = r + 1
            for p in which:
                center = state[now, p, q, middle, :]
                low0 = state[now, p - 1, q, middle, :]
                high0 = state[now, p + 1, q, middle, :]
                low1 = state[now, p, q - 1, middle, :]
                high1 = state[now, p, q + 1, middle, :]
                low2 = state[now, p, q, pl.ds(PAD - 1, depth), :]
                high2 = state[now, p, q, pl.ds(PAD + 1, depth), :]
                spread = low0 + high0 + low1 + high1 + low2 + high2 - 6.0 * center
                state[later, p, q, middle, :] = (
                    center
                    - winds[0, p - 1, r] * (high0 - low0)
                    - winds[1, p - 1, r] * (high1 - low1)
                    - winds[2, p - 1, r] * (high2 - low2)
                    + SMOOTH * spread
                )
            return carry

        lax.fori_loop(0, per, row, 0)

    def start_all(copies):
        for copy in copies:
            copy.start()

    start_all(south_copies(0, 0))
    start_all((east_copy(0, 0), east_copy(0, 1)))

    def first_sends(c, carry):
        start_all(down_copies(0, c))

        @pl.when(c > 0)
        def _():
            start_all(south_copies(0, c))

        return carry

    lax.fori_loop(0, CHUNKS, first_sends, 0)

    for load in loads:
        load.wait()

    edges = (1, planes)
    inner = tuple(range(2, planes))

    for n in range(STEPS):
        for way in (0, 1):
            east_copy(n, way).wait_recv()
            if n > 0:
                east_copy(n - 1, way).wait_send()

        def chunk(c, carry, n=n):
            for copy in down_copies(n, c):
                copy.wait_recv()
            if n > 0:
                for copy in south_copies(n - 1, c) + down_copies(n - 1, c):
                    copy.wait_send()
            if n == STEPS - 1:
                compute(n, c, inner)
            for copy in south_copies(n, c):
                copy.wait_recv()
            compute(n, c, edges)
            if n == STEPS - 1:
                out_copy(c).start()
            else:
                compute(n, c, inner)
                start_all(south_copies(n + 1, c))
                start_all(down_copies(n + 1, c))

                @pl.when(c == 0)
                def _():
                    east_copy(n + 1, 1).start()

                @pl.when(c == CHUNKS - 1)
                def _():
                    east_copy(n + 1, 0).start()

            return carry

        lax.fori_loop(0, CHUNKS, chunk, 0)

    def finish(c, carry):
        for copy in south_copies(STEPS - 1, c) + down_copies(STEPS - 1, c):
            copy.wait_send()
        out_copy(c).wait()
        return carry

    lax.fori_loop(0, CHUNKS, finish, 0)
    for way in (0, 1):
        east_copy(STEPS - 1, way).wait_send()


def solution(mesh):
    sizes = tuple(mesh.shape[a] for a in ("south", "east", "down"))
    spec = P("south", "east", "down", None)

    def on_device(x, wind_south, wind_east, wind_down):
        planes, rows, depth, levels = x.shape
        dma = pltpu.SemaphoreType.DMA
        return pl.pallas_call(
            functools.partial(kernel, sizes),
            out_shape=jax.ShapeDtypeStruct(x.shape, x.dtype),
            in_specs=[pl.BlockSpec(memory_space=pl.ANY)] * 4,
            out_specs=pl.BlockSpec(memory_space=pl.ANY),
            scratch_shapes=[
                pltpu.VMEM((2, planes + 2, rows + 2, depth + 2 * PAD, levels), x.dtype),
                pltpu.VMEM((3, planes, rows, depth, levels), x.dtype),
                dma((4, planes)),
                dma((2, STEPS, CHUNKS)),
                dma((2, STEPS, CHUNKS)),
                dma((2, STEPS)),
                dma((2, STEPS)),
                dma((2, STEPS, CHUNKS)),
                dma((2, STEPS, CHUNKS)),
                dma((CHUNKS,)),
            ],
            compiler_params=pltpu.CompilerParams(
                collective_id=0, has_side_effects=True, vmem_limit_bytes=60 * 1024 * 1024
            ),
            name="advect",
        )(x, wind_south, wind_east, wind_down)

    return jax.shard_map(on_device, mesh=mesh, in_specs=(spec,) * 4, out_specs=spec, check_vma=False)
```

```python
import functools

import jax
from jax import lax
from jax.experimental import pallas as pl
from jax.experimental.pallas import tpu as pltpu
from jax.sharding import PartitionSpec as P

STEPS = 4
PARTS = (14, 14, 2, 2)
PAD = 8
MESH = pl.DeviceIdType.MESH
SMOOTH = 0.05


def kernel(
    sizes,
    parts,
    x_hbm,
    wind_south_hbm,
    wind_east_hbm,
    wind_down_hbm,
    out,
    state,
    winds,
    load_sem,
    south_send,
    south_recv,
    east_send,
    east_recv,
    down_send,
    down_recv,
):
    n_south, n_east, n_down = sizes
    planes, rows, depth, _ = x_hbm.shape
    middle = pl.ds(PAD, depth)
    own_planes = pl.ds(1, planes)

    me_south, me_east, me_down = (lax.axis_index(a) for a in ("south", "east", "down"))
    above = {"south": lax.rem(me_south + 1, n_south)}
    below = {"south": lax.rem(me_south + n_south - 1, n_south)}
    right = {"east": lax.rem(me_east + 1, n_east)}
    left = {"east": lax.rem(me_east + n_east - 1, n_east)}
    partner = {"down": lax.rem(me_down + 1, n_down)}

    barrier = pltpu.get_barrier_semaphore()
    for neighbour in (above, below, right, left, partner):
        pl.semaphore_signal(barrier, inc=1, device_id=neighbour, device_id_type=MESH)
    pl.semaphore_wait(barrier, 5)

    def remote(src, dst, send, recv, device):
        return pltpu.make_async_remote_copy(
            src_ref=src, dst_ref=dst, send_sem=send, recv_sem=recv, device_id=device, device_id_type=MESH
        )

    def south_copies(n, c):
        slot = n % 2
        first, size = parts[c]
        here = pl.ds(1 + first, size)
        result = []
        for way, (p, halo, device) in enumerate(((planes, 0, above), (1, planes + 1, below))):
            if n == 0:
                src = x_hbm.at[p - 1, pl.ds(first, size)]
            else:
                src = state.at[slot, p, here, middle]
            dst = state.at[slot, halo, here, middle]
            result.append(remote(src, dst, south_send.at[way, n, c], south_recv.at[way, n, c], device))
        return result

    def east_copy(n, way):
        slot = n % 2
        r, halo, device = ((rows, 0, right), (1, rows + 1, left))[way]
        src = x_hbm.at[:, r - 1] if n == 0 else state.at[slot, own_planes, r, middle]
        dst = state.at[slot, own_planes, halo, middle]
        return remote(src, dst, east_send.at[way, n], east_recv.at[way, n], device)

    def down_copies(n, c):
        slot = n % 2
        first, size = parts[c]
        here = pl.ds(1 + first, size)
        result = []
        for way, (k, halo) in enumerate(((depth - PAD, 0), (0, depth + PAD))):
            if n == 0:
                src = x_hbm.at[:, pl.ds(first, size), pl.ds(k, PAD)]
            else:
                src = state.at[slot, own_planes, here, pl.ds(PAD + k, PAD)]
            dst = state.at[slot, own_planes, here, pl.ds(halo, PAD)]
            result.append(remote(src, dst, down_send.at[way, n, c], down_recv.at[way, n, c], partner))
        return result

    def compute(n, c, which):
        now, later = n % 2, (n + 1) % 2
        first, size = parts[c]

        def row(r, carry):
            q = r + 1
            for p in which:
                center = state[now, p, q, middle, :]
                low0 = state[now, p - 1, q, middle, :]
                high0 = state[now, p + 1, q, middle, :]
                low1 = state[now, p, q - 1, middle, :]
                high1 = state[now, p, q + 1, middle, :]
                low2 = state[now, p, q, pl.ds(PAD - 1, depth), :]
                high2 = state[now, p, q, pl.ds(PAD + 1, depth), :]
                spread = low0 + high0 + low1 + high1 + low2 + high2 - 6.0 * center
                value = (
                    center
                    - winds[0, p - 1, r] * (high0 - low0)
                    - winds[1, p - 1, r] * (high1 - low1)
                    - winds[2, p - 1, r] * (high2 - low2)
                    + SMOOTH * spread
                )
                if n == STEPS - 1:
                    out[p - 1, r] = value
                else:
                    state[later, p, q, middle, :] = value
            return carry

        lax.fori_loop(first, first + size, row, 0)

    def start_all(copies):
        for copy in copies:
            copy.start()

    count = len(parts)
    for c in range(count):
        start_all(south_copies(0, c))
        if c == 0:
            start_all((east_copy(0, 0), east_copy(0, 1)))
        start_all(down_copies(0, c))

    loads = []
    for a, ref in enumerate((x_hbm, wind_south_hbm, wind_east_hbm, wind_down_hbm)):
        for p in range(planes):
            target = state.at[0, 1 + p, pl.ds(1, rows), middle] if a == 0 else winds.at[a - 1, p]
            loads.append(pltpu.make_async_copy(ref.at[p], target, load_sem.at[a, p]))
    start_all(loads)
    for load in loads:
        load.wait()

    edges = (1, planes)
    inner = tuple(range(2, planes))

    for n in range(STEPS):
        last = n == STEPS - 1
        for way in (0, 1):
            east_copy(n, way).wait_recv()
            if n > 0:
                east_copy(n - 1, way).wait_send()

        for c in range(count):
            for copy in down_copies(n, c):
                copy.wait_recv()
            if n > 0:
                for copy in south_copies(n - 1, c) + down_copies(n - 1, c):
                    copy.wait_send()
            if last:
                compute(n, c, inner)
            for copy in south_copies(n, c):
                copy.wait_recv()
            compute(n, c, edges)
            if not last:
                compute(n, c, inner)
                start_all(south_copies(n + 1, c))
                start_all(down_copies(n + 1, c))
                if c == 0:
                    east_copy(n + 1, 1).start()
                if c == count - 1:
                    east_copy(n + 1, 0).start()

    for c in range(count):
        for copy in south_copies(STEPS - 1, c) + down_copies(STEPS - 1, c):
            copy.wait_send()
    for way in (0, 1):
        east_copy(STEPS - 1, way).wait_send()


def solution(mesh):
    sizes = tuple(mesh.shape[a] for a in ("south", "east", "down"))
    spec = P("south", "east", "down", None)

    def on_device(x, wind_south, wind_east, wind_down):
        planes, rows, depth, levels = x.shape
        parts, first = [], 0
        for share in PARTS:
            parts.append((first, share * rows // sum(PARTS)))
            first += parts[-1][1]
        dma = pltpu.SemaphoreType.DMA
        return pl.pallas_call(
            functools.partial(kernel, sizes, tuple(parts)),
            out_shape=pltpu.VMEM(x.shape, x.dtype),
            in_specs=[pl.BlockSpec(memory_space=pltpu.HBM)] * 4,
            out_specs=pl.BlockSpec(memory_space=pltpu.VMEM),
            scratch_shapes=[
                pltpu.VMEM((2, planes + 2, rows + 2, depth + 2 * PAD, levels), x.dtype),
                pltpu.VMEM((3, planes, rows, depth, levels), x.dtype),
                dma((4, planes)),
                dma((2, STEPS, len(parts))),
                dma((2, STEPS, len(parts))),
                dma((2, STEPS)),
                dma((2, STEPS)),
                dma((2, STEPS, len(parts))),
                dma((2, STEPS, len(parts))),
            ],
            compiler_params=pltpu.CompilerParams(
                collective_id=0, has_side_effects=True, vmem_limit_bytes=54 * 1024 * 1024
            ),
            name="advect",
        )(x, wind_south, wind_east, wind_down)

    return jax.shard_map(on_device, mesh=mesh, in_specs=(spec,) * 4, out_specs=spec, check_vma=False)
```

```python
import functools

import jax
from jax import lax
from jax.experimental import pallas as pl
from jax.experimental.pallas import tpu as pltpu
from jax.sharding import PartitionSpec as P

STEPS = 4
PARTS = (2, 14, 14, 2)
PAD = 8
MESH = pl.DeviceIdType.MESH
SMOOTH = 0.05


def kernel(
    sizes,
    parts,
    x_hbm,
    wind_south_hbm,
    wind_east_hbm,
    wind_down_hbm,
    out,
    state,
    winds,
    load_sem,
    south_send,
    south_recv,
    east_send,
    east_recv,
    down_send,
    down_recv,
):
    n_south, n_east, n_down = sizes
    planes, rows, depth, _ = x_hbm.shape
    middle = pl.ds(PAD, depth)
    own_planes = pl.ds(1, planes)

    me_south, me_east, me_down = (lax.axis_index(a) for a in ("south", "east", "down"))
    above = {"south": lax.rem(me_south + 1, n_south)}
    below = {"south": lax.rem(me_south + n_south - 1, n_south)}
    right = {"east": lax.rem(me_east + 1, n_east)}
    left = {"east": lax.rem(me_east + n_east - 1, n_east)}
    partner = {"down": lax.rem(me_down + 1, n_down)}

    first, size = parts[0]
    heads = [
        pltpu.make_async_copy(
            x_hbm.at[p - 1, pl.ds(first, size)], state.at[0, p, pl.ds(1 + first, size), middle], load_sem.at[i]
        )
        for i, p in ((0, planes), (1, 1))
    ]
    for head in heads:
        head.start()

    barrier = pltpu.get_barrier_semaphore()
    for neighbour in (above, below, right, left, partner):
        pl.semaphore_signal(barrier, inc=1, device_id=neighbour, device_id_type=MESH)
    pl.semaphore_wait(barrier, 5)

    def remote(src, dst, send, recv, device):
        return pltpu.make_async_remote_copy(
            src_ref=src, dst_ref=dst, send_sem=send, recv_sem=recv, device_id=device, device_id_type=MESH
        )

    def south_copies(n, c):
        slot = n % 2
        first, size = parts[c]
        here = pl.ds(1 + first, size)
        result = []
        for way, (p, halo, device) in enumerate(((planes, 0, above), (1, planes + 1, below))):
            if n == 0 and c > 0:
                src = x_hbm.at[p - 1, pl.ds(first, size)]
            else:
                src = state.at[slot, p, here, middle]
            dst = state.at[slot, halo, here, middle]
            result.append(remote(src, dst, south_send.at[way, slot, c], south_recv.at[way, slot, c], device))
        return result

    def east_copy(n, way):
        slot = n % 2
        r, halo, device = ((rows, 0, right), (1, rows + 1, left))[way]
        src = x_hbm.at[:, r - 1] if n == 0 else state.at[slot, own_planes, r, middle]
        dst = state.at[slot, own_planes, halo, middle]
        return remote(src, dst, east_send.at[way, slot], east_recv.at[way, slot], device)

    def down_copies(n):
        slot = n % 2
        here = pl.ds(1, rows)
        result = []
        for way, (k, halo) in enumerate(((depth - PAD, 0), (0, depth + PAD))):
            if n == 0:
                src = x_hbm.at[:, :, pl.ds(k, PAD)]
            else:
                src = state.at[slot, own_planes, here, pl.ds(PAD + k, PAD)]
            dst = state.at[slot, own_planes, here, pl.ds(halo, PAD)]
            result.append(remote(src, dst, down_send.at[way, slot], down_recv.at[way, slot], partner))
        return result

    def compute(n, c, which):
        now, later = n % 2, (n + 1) % 2
        first, size = parts[c]

        def row(r, carry):
            q = r + 1
            for p in which:
                center = state[now, p, q, middle, :]
                low0 = state[now, p - 1, q, middle, :]
                high0 = state[now, p + 1, q, middle, :]
                low1 = state[now, p, q - 1, middle, :]
                high1 = state[now, p, q + 1, middle, :]
                low2 = state[now, p, q, pl.ds(PAD - 1, depth), :]
                high2 = state[now, p, q, pl.ds(PAD + 1, depth), :]
                spread = low0 + high0 + low1 + high1 + low2 + high2 - 6.0 * center
                value = (
                    center
                    - winds[0, p - 1, r] * (high0 - low0)
                    - winds[1, p - 1, r] * (high1 - low1)
                    - winds[2, p - 1, r] * (high2 - low2)
                    + SMOOTH * spread
                )
                if n == STEPS - 1:
                    out[p - 1, r] = value
                else:
                    state[later, p, q, middle, :] = value
            return carry

        lax.fori_loop(first, first + size, row, 0)

    def start_all(copies):
        for copy in copies:
            copy.start()

    count = len(parts)
    for head in heads:
        head.wait()
    for c in range(count):
        start_all(south_copies(0, c))
        if c == 0:
            start_all((east_copy(0, 0), east_copy(0, 1)))
            start_all(down_copies(0))

    rest = rows - size
    loads = [
        pltpu.make_async_copy(
            x_hbm.at[:, pl.ds(size, rest)], state.at[0, own_planes, pl.ds(1 + size, rest), middle], load_sem.at[0]
        ),
        pltpu.make_async_copy(
            x_hbm.at[pl.ds(1, planes - 2), pl.ds(0, size)],
            state.at[0, pl.ds(2, planes - 2), pl.ds(1, size), middle],
            load_sem.at[4],
        ),
    ]
    for d, ref in enumerate((wind_south_hbm, wind_east_hbm, wind_down_hbm)):
        loads.append(pltpu.make_async_copy(ref, winds.at[d], load_sem.at[1 + d]))
    start_all(loads)
    for load in loads:
        load.wait()

    edges = (1, planes)
    inner = tuple(range(2, planes))

    for n in range(STEPS):
        last = n == STEPS - 1
        for copy in [east_copy(n, 0), east_copy(n, 1)] + down_copies(n):
            copy.wait_recv()
        if n > 0:
            for copy in [east_copy(n - 1, 0), east_copy(n - 1, 1)] + down_copies(n - 1):
                copy.wait_send()

        for c in range(count):
            if n > 0:
                for copy in south_copies(n - 1, c):
                    copy.wait_send()
            if last:
                compute(n, c, inner)
            for copy in south_copies(n, c):
                copy.wait_recv()
            compute(n, c, edges)
            if not last:
                compute(n, c, inner)
                start_all(south_copies(n + 1, c))
                if c == 0:
                    east_copy(n + 1, 1).start()
                if c == count - 1:
                    east_copy(n + 1, 0).start()
                    start_all(down_copies(n + 1))

    for c in range(count):
        for copy in south_copies(STEPS - 1, c):
            copy.wait_send()
    for copy in [east_copy(STEPS - 1, 0), east_copy(STEPS - 1, 1)] + down_copies(STEPS - 1):
        copy.wait_send()


def solution(mesh):
    sizes = tuple(mesh.shape[a] for a in ("south", "east", "down"))
    spec = P("south", "east", "down", None)

    def on_device(x, wind_south, wind_east, wind_down):
        planes, rows, depth, levels = x.shape
        parts, first = [], 0
        for share in PARTS:
            parts.append((first, share * rows // sum(PARTS)))
            first += parts[-1][1]
        dma = pltpu.SemaphoreType.DMA
        return pl.pallas_call(
            functools.partial(kernel, sizes, tuple(parts)),
            out_shape=pltpu.VMEM(x.shape, x.dtype),
            in_specs=[pl.BlockSpec(memory_space=pltpu.HBM)] * 4,
            out_specs=pl.BlockSpec(memory_space=pltpu.VMEM),
            scratch_shapes=[
                pltpu.VMEM((2, planes + 2, rows + 2, depth + 2 * PAD, levels), x.dtype),
                pltpu.VMEM((3, planes, rows, depth, levels), x.dtype),
                dma((5,)),
                dma((2, 2, len(parts))),
                dma((2, 2, len(parts))),
                dma((2, 2)),
                dma((2, 2)),
                dma((2, 2)),
                dma((2, 2)),
            ],
            compiler_params=pltpu.CompilerParams(
                collective_id=0, has_side_effects=True, vmem_limit_bytes=54 * 1024 * 1024
            ),
            name="advect",
        )(x, wind_south, wind_east, wind_down)

    return jax.shard_map(on_device, mesh=mesh, in_specs=(spec,) * 4, out_specs=spec, check_vma=False)
```

```python
import functools

import jax
import jax.numpy as jnp
from jax import lax
from jax.experimental import pallas as pl
from jax.experimental.pallas import tpu as pltpu
from jax.sharding import PartitionSpec as P

STEPS = 4
PARTS = (
    ((2, 0), (14, 1), (16, 2)),
    ((16, 3), (16, 4)),
    ((16, 0), (16, 2)),
    ((14, 3), (16, 4), (2, 1)),
)
FACE_SEMAPHORES = 6
PAD = 8
MESH = pl.DeviceIdType.MESH
SMOOTH = 0.05


def kernel(
    sizes,
    parts,
    x_hbm,
    wind_south_hbm,
    wind_east_hbm,
    wind_down_hbm,
    out,
    state,
    winds,
    load_sem,
    south_send,
    south_recv,
    east_send,
    east_recv,
    down_send,
    down_recv,
    told,
):
    n_south, n_east, n_down = sizes
    planes, rows, depth, _ = x_hbm.shape
    middle = pl.ds(PAD, depth)
    own_planes = pl.ds(1, planes)

    me_south, me_east, me_down = (lax.axis_index(a) for a in ("south", "east", "down"))
    above = {"south": lax.rem(me_south + 1, n_south)}
    below = {"south": lax.rem(me_south + n_south - 1, n_south)}
    right = {"east": lax.rem(me_east + 1, n_east)}
    left = {"east": lax.rem(me_east + n_east - 1, n_east)}
    partner = {"down": lax.rem(me_down + 1, n_down)}

    first, size, _ = parts[0][0]
    heads = [
        pltpu.make_async_copy(
            x_hbm.at[p - 1, pl.ds(first, size)], state.at[0, p, pl.ds(1 + first, size), middle], load_sem.at[i]
        )
        for i, p in ((0, planes), (1, 1))
    ]
    for head in heads:
        head.start()

    barrier = pltpu.get_barrier_semaphore()
    for neighbour in ({**above, "down": 0}, below, {**right, "down": 0}, {**left, "down": 0}):
        pl.semaphore_signal(barrier, inc=1, device_id=neighbour, device_id_type=MESH)

    @pl.when(me_down == 1)
    def _():
        pl.semaphore_signal(barrier, inc=1, device_id=partner, device_id_type=MESH)

    pl.semaphore_wait(barrier, jnp.where(me_down == 1, 1, 8))

    @pl.when(me_down == 0)
    def _():
        pl.semaphore_signal(told, inc=1, device_id=partner, device_id_type=MESH)


    def remote(src, dst, send, recv, device):
        return pltpu.make_async_remote_copy(
            src_ref=src, dst_ref=dst, send_sem=send, recv_sem=recv, device_id=device, device_id_type=MESH
        )

    def south_copies(n, c, ways=(0, 1)):
        slot = n % 2
        first, size, sem = parts[n][c]
        here = pl.ds(1 + first, size)
        result = []
        for way in ways:
            p, halo, device = ((planes, 0, above), (1, planes + 1, below))[way]
            if n == 0 and c > 0:
                src = x_hbm.at[p - 1, pl.ds(first, size)]
            else:
                src = state.at[slot, p, here, middle]
            dst = state.at[slot, halo, here, middle]
            result.append(remote(src, dst, south_send.at[way, sem], south_recv.at[way, sem], device))
        return result

    def east_copy(n, way):
        slot = n % 2
        r, halo, device = ((rows, 0, right), (1, rows + 1, left))[way]
        src = x_hbm.at[:, r - 1] if n == 0 else state.at[slot, own_planes, r, middle]
        dst = state.at[slot, own_planes, halo, middle]
        return remote(src, dst, east_send.at[way, slot], east_recv.at[way, slot], device)

    def down_copies(n):
        slot = n % 2
        here = pl.ds(1, rows)
        result = []
        for way, (k, halo) in enumerate(((depth - PAD, 0), (0, depth + PAD))):
            if n == 0:
                src = x_hbm.at[:, :, pl.ds(k, PAD)]
            else:
                src = state.at[slot, own_planes, here, pl.ds(PAD + k, PAD)]
            dst = state.at[slot, own_planes, here, pl.ds(halo, PAD)]
            result.append(remote(src, dst, down_send.at[way, slot], down_recv.at[way, slot], partner))
        return result

    def compute(n, c, which):
        now, later = n % 2, (n + 1) % 2
        first, size, _ = parts[n][c]

        def row(r, carry):
            q = r + 1
            for p in which:
                center = state[now, p, q, middle, :]
                low0 = state[now, p - 1, q, middle, :]
                high0 = state[now, p + 1, q, middle, :]
                low1 = state[now, p, q - 1, middle, :]
                high1 = state[now, p, q + 1, middle, :]
                low2 = state[now, p, q, pl.ds(PAD - 1, depth), :]
                high2 = state[now, p, q, pl.ds(PAD + 1, depth), :]
                spread = low0 + high0 + low1 + high1 + low2 + high2 - 6.0 * center
                value = (
                    center
                    - winds[0, p - 1, r] * (high0 - low0)
                    - winds[1, p - 1, r] * (high1 - low1)
                    - winds[2, p - 1, r] * (high2 - low2)
                    + SMOOTH * spread
                )
                if n == STEPS - 1:
                    out[p - 1, r] = value
                else:
                    state[later, p, q, middle, :] = value
            return carry

        lax.fori_loop(first, first + size, row, 0)

    def start_all(copies):
        for copy in copies:
            copy.start()

    for head in heads:
        head.wait()
    for c in range(len(parts[0])):
        start_all(south_copies(0, c, (0,)))

    @pl.when(me_down == 1)
    def _():
        pl.semaphore_wait(told, 1)

    for c in range(len(parts[0])):
        start_all(south_copies(0, c, (1,)))
    start_all((east_copy(0, 0), east_copy(0, 1)))
    start_all(down_copies(0))

    rest = rows - size
    loads = [
        pltpu.make_async_copy(
            x_hbm.at[:, pl.ds(size, rest)], state.at[0, own_planes, pl.ds(1 + size, rest), middle], load_sem.at[0]
        ),
        pltpu.make_async_copy(
            x_hbm.at[pl.ds(1, planes - 2), pl.ds(0, size)],
            state.at[0, pl.ds(2, planes - 2), pl.ds(1, size), middle],
            load_sem.at[4],
        ),
    ]
    for d, ref in enumerate((wind_south_hbm, wind_east_hbm, wind_down_hbm)):
        loads.append(pltpu.make_async_copy(ref, winds.at[d], load_sem.at[1 + d]))
    start_all(loads)
    for load in loads:
        load.wait()

    edges = (1, planes)
    inner = tuple(range(2, planes))
    ready = [list(range(len(step))) for step in parts]
    sent = [list(range(len(step))) for step in parts]

    for n in range(STEPS):
        last = n == STEPS - 1
        for copy in [east_copy(n, 0), east_copy(n, 1)] + down_copies(n):
            copy.wait_recv()
        if n > 0:
            for copy in [east_copy(n - 1, 0), east_copy(n - 1, 1)] + down_copies(n - 1):
                copy.wait_send()

        count = len(parts[n])
        for c in range(count):
            end = parts[n][c][0] + parts[n][c][1]
            if 0 < n and not last:
                while sent[n - 1] and parts[n - 1][sent[n - 1][0]][0] < end:
                    for copy in south_copies(n - 1, sent[n - 1].pop(0)):
                        copy.wait_send()
            if last:
                compute(n, c, inner)
            for copy in south_copies(n, c):
                copy.wait_recv()
            compute(n, c, edges)
            if not last:
                compute(n, c, inner)
                while ready[n + 1] and sum(parts[n + 1][ready[n + 1][0]][:2]) <= end:
                    start_all(south_copies(n + 1, ready[n + 1].pop(0)))
                if c == 0:
                    east_copy(n + 1, 1).start()
                if c == count - 1:
                    east_copy(n + 1, 0).start()
                    start_all(down_copies(n + 1))

    for n in range(STEPS):
        for c in sent[n]:
            for copy in south_copies(n, c):
                copy.wait_send()
    for copy in [east_copy(STEPS - 1, 0), east_copy(STEPS - 1, 1)] + down_copies(STEPS - 1):
        copy.wait_send()


def solution(mesh):
    sizes = tuple(mesh.shape[a] for a in ("south", "east", "down"))
    spec = P("south", "east", "down", None)

    def on_device(x, wind_south, wind_east, wind_down):
        planes, rows, depth, levels = x.shape
        parts = []
        for step in PARTS:
            parts.append([])
            first = 0
            for share, semaphore in step:
                size = share * rows // 32
                parts[-1].append((first, size, semaphore))
                first += size
        dma = pltpu.SemaphoreType.DMA
        return pl.pallas_call(
            functools.partial(kernel, sizes, parts),
            out_shape=pltpu.VMEM(x.shape, x.dtype),
            in_specs=[pl.BlockSpec(memory_space=pltpu.HBM)] * 4,
            out_specs=pl.BlockSpec(memory_space=pltpu.VMEM),
            scratch_shapes=[
                pltpu.VMEM((2, planes + 2, rows + 2, depth + 2 * PAD, levels), x.dtype),
                pltpu.VMEM((3, planes, rows, depth, levels), x.dtype),
                dma((5,)),
                dma((2, FACE_SEMAPHORES)),
                dma((2, FACE_SEMAPHORES)),
                dma((2, 2)),
                dma((2, 2)),
                dma((2, 2)),
                dma((2, 2)),
                pltpu.SemaphoreType.REGULAR,
            ],
            compiler_params=pltpu.CompilerParams(
                collective_id=0, has_side_effects=True, vmem_limit_bytes=54 * 1024 * 1024
            ),
            name="advect",
        )(x, wind_south, wind_east, wind_down)

    return jax.shard_map(on_device, mesh=mesh, in_specs=(spec,) * 4, out_specs=spec, check_vma=False)
```
